16 devices in a mesh: dp: 1, tp: 16 (over x, y, z, core).
Axes of the slice: x: 2, y: 2, z: 2, core: 2. Of those that a mesh axis runs over, the one named last changes fastest.
Arguments:
- x: bfloat16 [2048, 5120], P('dp')
- dy: bfloat16 [2048, 5120], P('dp')
- gate: bfloat16 [2048, 16384], P('dp', 'tp')
- up: bfloat16 [2048, 16384], P('dp', 'tp')
- w_gate: bfloat16 [5120, 16384], P(None, 'tp')
- w_up: bfloat16 [5120, 16384], P(None, 'tp')
- w_down: bfloat16 [16384, 5120], P('tp')
Outputs:
- output 1: bfloat16 [2048, 5120], P('dp')
- output 2: bfloat16 [5120, 16384], P('dp', 'tp')
- output 3: bfloat16 [5120, 16384], P('dp', 'tp')
- output 4: bfloat16 [16384, 5120], P(('dp', 'tp'))
All inputs are finite; a program needn't handle non-finite values.
Results may differ from the reference program's by a relative error of at most 0.012.
Values are sent between devices in bfloat16 or wider.
A program may use at most 2 GiB of HBM per device.

```python
import jax
import jax.numpy as jnp

ROWS = 2048
D = 5120
FF = 16384


def act(gate, up):
    return jax.nn.silu(gate) * up


def setup_inputs(seed: int = 0, part: int = 0) -> dict:
    kx, ky, ka, kb, kg, ku, kd = jax.random.split(jax.random.key(seed), 7)
    kx, ky, ka, kb = (jax.random.fold_in(k, part) for k in (kx, ky, ka, kb))
    drawn = {
        "x": jax.random.normal(kx, (ROWS, D), jnp.float32),
        "dy": jax.random.normal(ky, (ROWS, D), jnp.float32),
        "gate": jax.random.normal(ka, (ROWS, FF), jnp.float32),
        "up": jax.random.normal(kb, (ROWS, FF), jnp.float32),
        "w_gate": jax.random.normal(kg, (D, FF), jnp.float32) * D**-0.5,
        "w_up": jax.random.normal(ku, (D, FF), jnp.float32) * D**-0.5,
        "w_down": jax.random.normal(kd, (FF, D), jnp.float32) * FF**-0.5,
    }
    return {k: v.astype(jnp.bfloat16) for k, v in drawn.items()}


def reference(x, dy, gate, up, w_gate, w_up, w_down):
    hidden, back = jax.vjp(act, gate.astype(jnp.float32), up.astype(jnp.float32))
    d_hidden = jnp.dot(dy, w_down.T, preferred_element_type=jnp.float32)
    d_gate, d_up = (g.astype(jnp.bfloat16) for g in back(d_hidden))
    dx = jnp.dot(d_gate, w_gate.T, preferred_element_type=jnp.float32) + jnp.dot(d_up, w_up.T, preferred_element_type=jnp.float32)
    dw_gate = jnp.dot(x.T, d_gate, preferred_element_type=jnp.float32)
    dw_up = jnp.dot(x.T, d_up, preferred_element_type=jnp.float32)
    dw_down = jnp.dot(hidden.astype(jnp.bfloat16).T, dy, preferred_element_type=jnp.float32)
    return tuple(g.astype(jnp.bfloat16) for g in (dx, dw_gate, dw_up, dw_down))
```

```python
import jax
import jax.numpy as jnp
from jax import lax
from jax.experimental import pallas as pl
from jax.experimental.pallas import tpu as pltpu
from jax.sharding import PartitionSpec as P

BF, F32 = jnp.bfloat16, jnp.float32
NT = (((1,), (1,)), ((), ()))
TN = (((0,), (0,)), ((), ()))
MESH = pl.DeviceIdType.MESH

ROWS, D, H = 2048, 5120, 1024
CHUNKS = 4
HALF = ROWS // CHUNKS // 2
Q1, Q2, Q3 = HALF // 2, HALF // 4, HALF // 8
COLS = ((0, 1792), (1792, 1792), (3584, 1536))
TILE = 512
TILES = D // TILE


def dot(a, b, dims):
    return lax.dot_general(a, b, dims, preferred_element_type=F32)


def kernel(x, dy, gate, up, w_gate, w_up, w_down, dx, dwg, dwu, dwd, dg_o, du_o, hd_o,
           acc1, acc2, acc3, ds_, dr, s1, r1, s2, r2, s3, r3, fin,
           d_s, d_r, p1_s, p1_r, p2_s, p2_r, p3_s, p3_r, loc_s,
           a1_s, a1_r, a2_s, a2_r, a3_s, a3_r, dd_s, dd_r):
    me, dp = lax.axis_index("tp"), lax.axis_index("dp")
    core, bz, by, bx = me % 2, me // 2 % 2, me // 4 % 2, me // 8 % 2
    other = me + 1 - 2 * core
    axes = {"x": (bx, me + 8 - 16 * bx), "y": (by, me + 4 - 8 * by), "z": (bz, me + 2 - 4 * bz)}
    orders = [[axes[a] for a in o] for o in ("xyz", "yzx", "zxy")]

    barrier = pltpu.get_barrier_semaphore()
    for peer in (other, axes["x"][1], axes["y"][1], axes["z"][1]):
        pl.semaphore_signal(barrier, inc=1, device_id=(dp, peer), device_id_type=MESH)
    pl.semaphore_wait(barrier, 4)

    def remote(src, dst, ss, rs, peer):
        return pltpu.make_async_remote_copy(src_ref=src, dst_ref=dst, send_sem=ss, recv_sem=rs,
                                            device_id=(dp, peer), device_id_type=MESH)

    def cols(j):
        return pl.ds(*COLS[j])

    def al(v, n):
        return pl.multiple_of(v, n)

    def base(c):
        return c * (2 * HALF) + HALF * core

    def d_copy(c, j):
        return remote(ds_.at[:, cols(j)], dr.at[c % 2, :, cols(j)], d_s.at[j], d_r.at[c % 2, j], other)

    def p1(c, j):
        return remote(s1.at[:, cols(j)], r1.at[c % 2, :, cols(j)], p1_s.at[j], p1_r.at[c % 2, j], orders[j][0][1])

    def p2(c, j):
        return remote(s2.at[c % 2, :, cols(j)], r2.at[c % 2, :, cols(j)], p2_s.at[c % 2, j], p2_r.at[c % 2, j], orders[j][1][1])

    def p3(c, j):
        return remote(s3.at[c % 2, :, cols(j)], r3.at[c % 2, :, cols(j)], p3_s.at[c % 2, j], p3_r.at[c % 2, j], orders[j][2][1])

    def rows3(c, j):
        b = orders[j]
        return pl.ds(al(base(c) + Q1 * b[0][0] + Q2 * b[1][0] + Q3 * b[2][0], Q3), Q3)

    def rows2(c, j):
        b = orders[j]
        return pl.ds(al(base(c) + Q1 * b[0][0] + Q2 * b[1][0], Q2), Q2)

    def rows1(c, j):
        return pl.ds(al(base(c) + Q1 * orders[j][0][0], Q1), Q1)

    def rows0(c):
        return pl.ds(al(base(c), HALF), HALF)

    def loc(c, j):
        return pltpu.make_async_copy(fin.at[c % 2, :, cols(j)], dx.at[rows3(c, j), cols(j)], loc_s.at[c % 2, j])

    def a1(c, j):
        return remote(fin.at[c % 2, :, cols(j)], dx.at[rows3(c, j), cols(j)], a1_s.at[c, j], a1_r.at[c, j], orders[j][2][1])

    def a2(c, j):
        r = dx.at[rows2(c, j), cols(j)]
        return remote(r, r, a2_s.at[c, j], a2_r.at[c, j], orders[j][1][1])

    def a3(c, j):
        r = dx.at[rows1(c, j), cols(j)]
        return remote(r, r, a3_s.at[c, j], a3_r.at[c, j], orders[j][0][1])

    def dd(c, j):
        r = dx.at[rows0(c), cols(j)]
        return remote(r, r, dd_s.at[c, j], dd_r.at[c, j], other)

    def stage1(c):
        for j in range(3):
            bit = orders[j][1][0]
            keep, send = pl.ds(al(Q2 * bit, Q2), Q2), pl.ds(al(Q2 - Q2 * bit, Q2), Q2)
            p1(c, j).wait_recv()

            @pl.when(c >= 2)
            def _():
                p2(c, j).wait_send()
            s2[c % 2, :, cols(j)] = (acc1[send, cols(j)] + r1[c % 2, send, cols(j)].astype(F32)).astype(BF)
            p2(c, j).start()
            acc2[:, cols(j)] = acc1[keep, cols(j)] + r1[c % 2, keep, cols(j)].astype(F32)

    def stage2(c):
        for j in range(3):
            bit = orders[j][2][0]
            keep, send = pl.ds(al(Q3 * bit, Q3), Q3), pl.ds(al(Q3 - Q3 * bit, Q3), Q3)
            p2(c, j).wait_recv()

            @pl.when(c >= 2)
            def _():
                p3(c, j).wait_send()
            s3[c % 2, :, cols(j)] = (acc2[send, cols(j)] + r2[c % 2, send, cols(j)].astype(F32)).astype(BF)
            p3(c, j).start()
            acc3[:, cols(j)] = acc2[keep, cols(j)] + r2[c % 2, keep, cols(j)].astype(F32)

    def stage3(c):
        for j in range(3):
            p3(c, j).wait_recv()

            @pl.when(c >= 2)
            def _():
                a1(c - 2, j).wait_send()
            fin[c % 2, :, cols(j)] = (acc3[:, cols(j)] + r3[c % 2, :, cols(j)].astype(F32)).astype(BF)
            a1(c, j).start()
            loc(c, j).start()

    def stage4(c):
        for j in range(3):
            loc(c, j).wait()
            a1(c, j).wait_recv()
            a2(c, j).start()

    def stage5(c):
        for j in range(3):
            a2(c, j).wait_recv()
            a3(c, j).start()

    def stage6(c):
        for j in range(3):
            a3(c, j).wait_recv()
            dd(c, j).start()

    def stage7(c):
        for j in range(3):
            dd(c, j).wait_recv()

    stages = (None, stage1, stage2, stage3, stage4, stage5, stage6, stage7)

    def terms_phase(wg, wu, wd, dyb, gb, ub, dgb, dub, hdb, ld_w, ld_wd, ld, wr):
        def start_rows(c, h):
            return c * (2 * HALF) + HALF * (core if h else 1 - core)

        def loads(c, h):
            r = pl.ds(al(start_rows(c, h), HALF), HALF)
            return [pltpu.make_async_copy(src.at[r], dst.at[h], ld.at[h, i])
                    for i, (src, dst) in enumerate(((dy, dyb), (gate, gb), (up, ub)))]

        def writes(c, h):
            r = pl.ds(al(start_rows(c, h), HALF), HALF)
            return [pltpu.make_async_copy(src.at[h], dst.at[r], wr.at[h, i])
                    for i, (src, dst) in enumerate(((dgb, dg_o), (dub, du_o), (hdb, hd_o)))]

        def weights(j):
            return [pltpu.make_async_copy(src.at[cols(j)], dst.at[cols(j)], ld_w.at[i, j])
                    for i, (src, dst) in enumerate(((w_gate, wg), (w_up, wu)))]

        for d in loads(0, 0):
            d.start()
        wd_load = pltpu.make_async_copy(w_down, wd, ld_wd)
        wd_load.start()
        for j in range(3):
            for d in weights(j):
                d.start()
        for d in loads(0, 1):
            d.start()
        wd_load.wait()

        def hidden_rows(c, h):
            for d in loads(c, h):
                d.wait()

            @pl.when(c >= 1)
            def _():
                for d in writes(c - 1, h):
                    d.wait()
            g, u = gb[h].astype(F32), ub[h].astype(F32)
            sig = jax.nn.sigmoid(g)
            silu = g * sig
            hdb[h] = (silu * u).astype(BF)
            dh = dot(dyb[h], wd[...], NT)
            dub[h] = (dh * silu).astype(BF)
            dgb[h] = (dh * u * (sig + silu * (1 - sig))).astype(BF)
            for d in writes(c, h):
                d.start()

            @pl.when(c + 1 < CHUNKS)
            def _():
                for d in loads(c + 1, h):
                    d.start()

        def term(h, j):
            return dot(dgb[h], wg[cols(j), :], NT) + dot(dub[h], wu[cols(j), :], NT)

        def chunk(c, carry):
            hidden_rows(c, 0)
            for j in range(3):
                @pl.when(c == 0)
                def _():
                    for d in weights(j):
                        d.wait()

                @pl.when(c >= 1)
                def _():
                    d_copy(c - 1, j).wait_send()
                ds_[:, cols(j)] = term(0, j).astype(BF)
                d_copy(c, j).start()

            @pl.when(c >= 2)
            def _():
                stage2(c - 2)
            hidden_rows(c, 1)

            @pl.when(c >= 1)
            def _():
                stage1(c - 1)

            @pl.when(c >= 3)
            def _():
                stage4(c - 3)
            for j in range(3):
                d_copy(c, j).wait_recv()

                @pl.when(c >= 1)
                def _():
                    p1(c - 1, j).wait_send()
                t = term(1, j) + dr[c % 2, :, cols(j)].astype(F32)
                high = orders[j][0][0] == 1
                s1[:, cols(j)] = jnp.where(high, t[:Q1], t[Q1:]).astype(BF)
                p1(c, j).start()
                acc1[:, cols(j)] = jnp.where(high, t[Q1:], t[:Q1])

            @pl.when(c >= 2)
            def _():
                stage3(c - 2)

            @pl.when(c >= 3)
            def _():
                stage5(c - 3)
            return carry

        lax.fori_loop(0, CHUNKS, chunk, 0)
        for h in range(2):
            for d in writes(CHUNKS - 1, h):
                d.wait()
        for j in range(3):
            d_copy(CHUNKS - 1, j).wait_send()

    bf = lambda *s: pltpu.VMEM(s, BF)
    dma = lambda *s: pltpu.SemaphoreType.DMA(s)
    pl.run_scoped(terms_phase, bf(D, H), bf(D, H), bf(H, D), bf(2, HALF, D), bf(2, HALF, H), bf(2, HALF, H),
                  bf(2, HALF, H), bf(2, HALF, H), bf(2, HALF, H), dma(2, 3), dma(), dma(2, 3), dma(2, 3))

    plan = {(0, 0): [(2, 2)], (1, 0): [(4, 1)], (1, 1): [(1, 3), (3, 2), (5, 1)], (2, 0): [(6, 0)],
            (2, 1): [(2, 3), (4, 2)], (3, 1): [(3, 3), (5, 2)], (4, 0): [(6, 1)], (4, 1): [(4, 3)],
            (5, 1): [(5, 3)], (6, 1): [(6, 2)], (8, 1): [(6, 3)]}

    def weights_phase(dg, du, hd, xb, yb, og, ou, od, ld_f, ld_x, ld_y, wr):
        def tile(t):
            return pl.ds(al(t * TILE, TILE), TILE)

        def load_x(t):
            return pltpu.make_async_copy(x.at[:, tile(t)], xb.at[t % 2], ld_x.at[t % 2])

        def load_y(t):
            return pltpu.make_async_copy(dy.at[:, tile(t)], yb.at[t % 2], ld_y.at[t % 2])

        full = [pltpu.make_async_copy(src, dst, ld_f.at[i])
                for i, (src, dst) in enumerate(((dg_o, dg), (du_o, du), (hd_o, hd)))]

        def writes(t):
            s = t % 2
            return [pltpu.make_async_copy(og.at[s], dwg.at[tile(t)], wr.at[s, 0]),
                    pltpu.make_async_copy(ou.at[s], dwu.at[tile(t)], wr.at[s, 1]),
                    pltpu.make_async_copy(od.at[s], dwd.at[:, tile(t)], wr.at[s, 2])]

        full[0].start()
        load_x(0).start()
        full[1].start()
        full[2].start()
        load_y(0).start()

        def unit(t, carry):
            s = t % 2

            @pl.when(t + 1 < TILES)
            def _():
                load_x(t + 1).start()
                load_y(t + 1).start()

            @pl.when(t >= 2)
            def _():
                for d in writes(t - 2):
                    d.wait()

            def serve(sub):
                for (tt, ss), todo in plan.items():
                    if ss == sub:
                        @pl.when(t == tt)
                        def _():
                            for k, c in todo:
                                stages[k](c)

            @pl.when(t == 0)
            def _():
                full[0].wait()
            load_x(t).wait()
            og[s] = dot(xb[s], dg[...], TN).astype(BF)
            writes(t)[0].start()

            @pl.when(t == 0)
            def _():
                full[1].wait()
            ou[s] = dot(xb[s], du[...], TN).astype(BF)
            writes(t)[1].start()
            serve(0)

            @pl.when(t == 0)
            def _():
                full[2].wait()
            load_y(t).wait()
            od[s] = dot(hd[...], yb[s], TN).astype(BF)
            writes(t)[2].start()
            serve(1)
            return carry

        lax.fori_loop(0, TILES, unit, 0)
        for t in (TILES - 2, TILES - 1):
            for d in writes(t):
                d.wait()

    pl.run_scoped(weights_phase, bf(ROWS, H), bf(ROWS, H), bf(ROWS, H), bf(2, ROWS, TILE), bf(2, ROWS, TILE),
                  bf(2, TILE, H), bf(2, TILE, H), bf(2, H, TILE), dma(3), dma(2), dma(2), dma(2, 3))

    for c in range(CHUNKS):
        stage7(c)
    for j in range(3):
        p1(CHUNKS - 1, j).wait_send()
        for c in (CHUNKS - 2, CHUNKS - 1):
            p2(c, j).wait_send()
            p3(c, j).wait_send()
            a1(c, j).wait_send()
        for c in range(CHUNKS):
            a2(c, j).wait_send()
            a3(c, j).wait_send()
            dd(c, j).wait_send()


def solution(mesh):
    bf = lambda *s: pltpu.VMEM(s, BF)
    dma = lambda *s: pltpu.SemaphoreType.DMA(s)

    def step(x, dy, gate, up, w_gate, w_up, w_down):
        outs = [(ROWS, D), (D, H), (D, H), (H, D), (ROWS, H), (ROWS, H), (ROWS, H)]
        scratch = [pltpu.VMEM((Q1, D), F32), pltpu.VMEM((Q2, D), F32), pltpu.VMEM((Q3, D), F32),
                   bf(HALF, D), bf(2, HALF, D), bf(Q1, D), bf(2, Q1, D), bf(2, Q2, D), bf(2, Q2, D),
                   bf(2, Q3, D), bf(2, Q3, D), bf(2, Q3, D),
                   dma(3), dma(2, 3), dma(3), dma(2, 3), dma(2, 3), dma(2, 3), dma(2, 3), dma(2, 3), dma(2, 3)]
        scratch += [dma(CHUNKS, 3)] * 8
        res = pl.pallas_call(
            kernel,
            in_specs=[pl.BlockSpec(memory_space=pl.ANY)] * 7,
            out_specs=[pl.BlockSpec(memory_space=pl.ANY)] * 7,
            out_shape=[jax.ShapeDtypeStruct(s, BF) for s in outs],
            scratch_shapes=scratch,
            compiler_params=pltpu.CompilerParams(collective_id=0, has_side_effects=True, vmem_limit_bytes=67043328),
        )(x, dy, gate, up, w_gate, w_up, w_down)
        return tuple(res[:4])

    tokens, columns, rows = P("dp", None), P(None, "tp"), P("tp", None)
    return jax.shard_map(
        step,
        mesh=mesh,
        in_specs=(tokens, tokens, P("dp", "tp"), P("dp", "tp"), columns, columns, rows),
        out_specs=(tokens, P("dp", "tp"), P("dp", "tp"), P(("dp", "tp"), None)),
        check_vma=False,
    )
```

```python
import functools

import jax
import jax.numpy as jnp
from jax import lax
from jax.experimental import pallas as pl
from jax.experimental.pallas import tpu as pltpu
from jax.sharding import PartitionSpec as P

BF, F32 = jnp.bfloat16, jnp.float32
NT = (((1,), (1,)), ((), ()))
TN = (((0,), (0,)), ((), ()))
MESH = pl.DeviceIdType.MESH

ROWS, D, H = 2048, 5120, 1024
CHUNKS = 4
HALF = ROWS // CHUNKS // 2
Q1, Q2, Q3 = HALF // 2, HALF // 4, HALF // 8
COLS = ((0, 1792), (1792, 1792), (3584, 1536))
TILE = 512
TILES = D // TILE

PLAN1 = {12: [100, 101, 102], 16: [200, 201, 202], 20: [110, 111, 112], 21: [300, 302], 24: [210, 212], 25: [301, 211], 27: [400], 28: [120, 122,
         121], 30: [310]}
PLAN2 = {0: [311, 221, 220], 2: [312, 222, 401, 130, 402], 3: [132], 4: [131], 5: [321], 6: [320, 322, 410, 412], 7: [411], 8: [230, 231, 232], 9:
         [420, 422], 10: [421], 11: [331, 501], 12: [330, 500], 13: [502], 15: [332], 16: [430, 431, 510], 18: [511, 512, 601], 19: [600, 602], 20:
         [432], 22: [520, 522], 23: [521, 610], 25: [611, 612], 26: [530, 532], 27: [531], 29: [620, 622]}
PLAN3 = [621, 632, 630, 631]


def dot(a, b, dims):
    return lax.dot_general(a, b, dims, preferred_element_type=F32)


def kernel(x, dy, gate, up, w_gate, w_up, w_down, dx, dwg, dwu, dwd, dg_o, du_o, hd_o,
           acc1, acc2, acc3, ds_, dr, s1, r1, s2, r2, s3, r3, fin,
           d_s, d_r, p1_s, p1_r, p2_s, p2_r, p3_s, p3_r, loc_s,
           a1_s, a1_r, a2_s, a2_r, a3_s, a3_r, dd_s, dd_r):
    me, dp = lax.axis_index("tp"), lax.axis_index("dp")
    core, bz, by, bx = me % 2, me // 2 % 2, me // 4 % 2, me // 8 % 2
    other = me + 1 - 2 * core
    axes = {"x": (bx, me + 8 - 16 * bx), "y": (by, me + 4 - 8 * by), "z": (bz, me + 2 - 4 * bz)}
    orders = [[axes[a] for a in o] for o in ("xyz", "yzx", "zxy")]

    barrier = pltpu.get_barrier_semaphore()
    for peer in (other, axes["x"][1], axes["y"][1], axes["z"][1]):
        pl.semaphore_signal(barrier, inc=1, device_id=(dp, peer), device_id_type=MESH)

    def remote(src, dst, ss, rs, peer):
        return pltpu.make_async_remote_copy(src_ref=src, dst_ref=dst, send_sem=ss, recv_sem=rs,
                                            device_id=(dp, peer), device_id_type=MESH)

    def cols(j):
        return pl.ds(*COLS[j])

    def al(v, n):
        return pl.multiple_of(v, n)

    def base(c):
        return c * (2 * HALF) + HALF * core

    def d_copy(c, j):
        return remote(ds_.at[:, cols(j)], dr.at[c % 2, :, cols(j)], d_s.at[j], d_r.at[c % 2, j], other)

    def p1(c, j):
        return remote(s1.at[:, cols(j)], r1.at[c % 2, :, cols(j)], p1_s.at[j], p1_r.at[c % 2, j], orders[j][0][1])

    def p2(c, j):
        return remote(s2.at[c % 2, :, cols(j)], r2.at[c % 2, :, cols(j)], p2_s.at[c % 2, j], p2_r.at[c % 2, j], orders[j][1][1])

    def p3(c, j):
        return remote(s3.at[c % 2, :, cols(j)], r3.at[c % 2, :, cols(j)], p3_s.at[c % 2, j], p3_r.at[c % 2, j], orders[j][2][1])

    def rows3(c, j):
        b = orders[j]
        return pl.ds(al(base(c) + Q1 * b[0][0] + Q2 * b[1][0] + Q3 * b[2][0], Q3), Q3)

    def rows2(c, j):
        b = orders[j]
        return pl.ds(al(base(c) + Q1 * b[0][0] + Q2 * b[1][0], Q2), Q2)

    def rows1(c, j):
        return pl.ds(al(base(c) + Q1 * orders[j][0][0], Q1), Q1)

    def rows0(c):
        return pl.ds(al(base(c), HALF), HALF)

    def loc(c, j):
        return pltpu.make_async_copy(fin.at[c % 2, :, cols(j)], dx.at[rows3(c, j), cols(j)], loc_s.at[c % 2, j])

    def a1(c, j):
        return remote(fin.at[c % 2, :, cols(j)], dx.at[rows3(c, j), cols(j)], a1_s.at[c, j], a1_r.at[c, j], orders[j][2][1])

    def a2(c, j):
        r = dx.at[rows2(c, j), cols(j)]
        return remote(r, r, a2_s.at[c, j], a2_r.at[c, j], orders[j][1][1])

    def a3(c, j):
        r = dx.at[rows1(c, j), cols(j)]
        return remote(r, r, a3_s.at[c, j], a3_r.at[c, j], orders[j][0][1])

    def dd(c, j):
        r = dx.at[rows0(c), cols(j)]
        return remote(r, r, dd_s.at[c, j], dd_r.at[c, j], other)

    def stage1(c, j):
        bit = orders[j][1][0]
        keep, send = pl.ds(al(Q2 * bit, Q2), Q2), pl.ds(al(Q2 - Q2 * bit, Q2), Q2)
        p1(c, j).wait_recv()
        if c >= 2:
            p2(c - 2, j).wait_send()
        s2[c % 2, :, cols(j)] = (acc1[send, cols(j)] + r1[c % 2, send, cols(j)].astype(F32)).astype(BF)
        p2(c, j).start()
        acc2[:, cols(j)] = acc1[keep, cols(j)] + r1[c % 2, keep, cols(j)].astype(F32)

    def stage2(c, j):
        bit = orders[j][2][0]
        keep, send = pl.ds(al(Q3 * bit, Q3), Q3), pl.ds(al(Q3 - Q3 * bit, Q3), Q3)
        p2(c, j).wait_recv()
        if c >= 2:
            p3(c - 2, j).wait_send()
        s3[c % 2, :, cols(j)] = (acc2[send, cols(j)] + r2[c % 2, send, cols(j)].astype(F32)).astype(BF)
        p3(c, j).start()
        acc3[:, cols(j)] = acc2[keep, cols(j)] + r2[c % 2, keep, cols(j)].astype(F32)

    def stage3(c, j):
        p3(c, j).wait_recv()
        if c >= 2:
            a1(c - 2, j).wait_send()
        fin[c % 2, :, cols(j)] = (acc3[:, cols(j)] + r3[c % 2, :, cols(j)].astype(F32)).astype(BF)
        a1(c, j).start()
        loc(c, j).start()

    def stage4(c, j):
        a1(c, j).wait_recv()
        loc(c, j).wait()
        a2(c, j).start()

    def stage5(c, j):
        a2(c, j).wait_recv()
        a3(c, j).start()

    def stage6(c, j):
        a3(c, j).wait_recv()
        dd(c, j).start()

    stages = (None, stage1, stage2, stage3, stage4, stage5, stage6)

    def run(codes):
        for code in codes:
            stages[code // 100](code // 10 % 10, code % 10)

    def serve(plan, per_step, step, sub):
        for at, codes in plan.items():
            if at % per_step == sub:
                pl.when(step == at // per_step)(functools.partial(run, codes))

    def terms_phase(wg, wu, wd, dyb, gb, ub, dgb, dub, hdb, ld_w, ld_wd, ld, wr):
        def start_rows(c, h):
            return c * (2 * HALF) + HALF * (core if h else 1 - core)

        def loads(c, h):
            r = pl.ds(al(start_rows(c, h), HALF), HALF)
            return [pltpu.make_async_copy(src.at[r], dst.at[h], ld.at[h, i])
                    for i, (src, dst) in enumerate(((dy, dyb), (gate, gb), (up, ub)))]

        def writes(c, h):
            r = pl.ds(al(start_rows(c, h), HALF), HALF)
            return [pltpu.make_async_copy(src.at[h], dst.at[r], wr.at[h, i])
                    for i, (src, dst) in enumerate(((dgb, dg_o), (dub, du_o), (hdb, hd_o)))]

        def weights(j):
            return [pltpu.make_async_copy(src.at[cols(j)], dst.at[cols(j)], ld_w.at[i, j])
                    for i, (src, dst) in enumerate(((w_gate, wg), (w_up, wu)))]

        halves = [pltpu.make_async_copy(w_down.at[pl.ds(i * (H // 2), H // 2)], wd.at[pl.ds(i * (H // 2), H // 2)], ld_wd.at[i])
                  for i in range(2)]
        for d in loads(0, 0) + halves:
            d.start()
        pl.semaphore_wait(barrier, 4)
        halves[0].wait()
        for d in weights(0):
            d.start()

        def hidden_rows(c, h):
            for d in loads(c, h):
                d.wait()

            @pl.when(c >= 1)
            def _():
                for d in writes(c - 1, h):
                    d.wait()
            for i in range(2):
                part = pl.ds(i * (H // 2), H // 2)
                if h == 0 and i == 1:
                    @pl.when(c == 0)
                    def _():
                        halves[1].wait()
                        for d in loads(0, 1) + weights(1) + weights(2):
                            d.start()
                g, u = gb[h, :, part].astype(F32), ub[h, :, part].astype(F32)
                sig = jax.nn.sigmoid(g)
                silu = g * sig
                hdb[h, :, part] = (silu * u).astype(BF)
                dh = dot(dyb[h], wd[part, :], NT)
                dub[h, :, part] = (dh * silu).astype(BF)
                dgb[h, :, part] = (dh * u * (sig + silu * (1 - sig))).astype(BF)
            for d in writes(c, h):
                d.start()

            @pl.when(c + 1 < CHUNKS)
            def _():
                for d in loads(c + 1, h):
                    d.start()

        def term(h, j):
            return dot(dgb[h], wg[cols(j), :], NT) + dot(dub[h], wu[cols(j), :], NT)

        def chunk(c, carry):
            hidden_rows(c, 0)
            serve(PLAN1, 8, c, 0)
            for j in range(3):
                @pl.when(c == 0)
                def _():
                    for d in weights(j):
                        d.wait()

                @pl.when(c >= 1)
                def _():
                    d_copy(c - 1, j).wait_send()
                ds_[:, cols(j)] = term(0, j).astype(BF)
                d_copy(c, j).start()
                serve(PLAN1, 8, c, 1 + j)
            hidden_rows(c, 1)
            serve(PLAN1, 8, c, 4)
            for j in range(3):
                d_copy(c, j).wait_recv()

                @pl.when(c >= 1)
                def _():
                    p1(c - 1, j).wait_send()
                t = term(1, j) + dr[c % 2, :, cols(j)].astype(F32)
                high = orders[j][0][0] == 1
                s1[:, cols(j)] = jnp.where(high, t[:Q1], t[Q1:]).astype(BF)
                p1(c, j).start()
                acc1[:, cols(j)] = jnp.where(high, t[Q1:], t[:Q1])
                serve(PLAN1, 8, c, 5 + j)
            return carry

        lax.fori_loop(0, CHUNKS, chunk, 0)
        for h in range(2):
            for d in writes(CHUNKS - 1, h):
                d.wait()
        for j in range(3):
            d_copy(CHUNKS - 1, j).wait_send()

    bf = lambda *s: pltpu.VMEM(s, BF)
    dma = lambda *s: pltpu.SemaphoreType.DMA(s)
    pl.run_scoped(terms_phase, bf(D, H), bf(D, H), bf(H, D), bf(2, HALF, D), bf(2, HALF, H), bf(2, HALF, H),
                  bf(2, HALF, H), bf(2, HALF, H), bf(2, HALF, H), dma(2, 3), dma(2), dma(2, 3), dma(2, 3))

    def weights_phase(dg, du, hd, xb, yb, og, ou, od, ld_f, ld_x, ld_y, wr):
        def tile(t):
            return pl.ds(al(t * TILE, TILE), TILE)

        def load_x(t):
            return pltpu.make_async_copy(x.at[:, tile(t)], xb.at[t % 2], ld_x.at[t % 2])

        def load_y(t):
            return pltpu.make_async_copy(dy.at[:, tile(t)], yb.at[t % 2], ld_y.at[t % 2])

        full = [pltpu.make_async_copy(src, dst, ld_f.at[i])
                for i, (src, dst) in enumerate(((dg_o, dg), (du_o, du), (hd_o, hd)))]

        def write(t, i):
            s = t % 2
            if i == 2:
                return pltpu.make_async_copy(od.at[s], dwd.at[:, tile(t)], wr.at[s, 2])
            src, dst = ((og, dwg), (ou, dwu))[i]
            return pltpu.make_async_copy(src.at[s], dst.at[tile(t)], wr.at[s, i])

        full[0].start()
        load_x(0).start()
        full[1].start()
        full[2].start()
        load_y(0).start()

        def unit(t, carry):
            s = t % 2

            @pl.when(t + 1 < TILES)
            def _():
                load_x(t + 1).start()
                load_y(t + 1).start()

            @pl.when(t >= 2)
            def _():
                for i in range(3):
                    write(t - 2, i).wait()

            for i, (out, full_v) in enumerate(((og, dg), (ou, du), (od, hd))):
                @pl.when(t == 0)
                def _():
                    full[i].wait()
                if i == 0:
                    load_x(t).wait()
                if i == 2:
                    load_y(t).wait()
                    out[s] = dot(full_v[...], yb[s], TN).astype(BF)
                else:
                    out[s] = dot(xb[s], full_v[...], TN).astype(BF)
                write(t, i).start()
                serve(PLAN2, 3, t, i)
            return carry

        lax.fori_loop(0, TILES, unit, 0)
        for t in (TILES - 2, TILES - 1):
            for i in range(3):
                write(t, i).wait()

    pl.run_scoped(weights_phase, bf(ROWS, H), bf(ROWS, H), bf(ROWS, H), bf(2, ROWS, TILE), bf(2, ROWS, TILE),
                  bf(2, TILE, H), bf(2, TILE, H), bf(2, H, TILE), dma(3), dma(2), dma(2), dma(2, 3))

    run(PLAN3)
    for j in range(3):
        for c in range(CHUNKS):
            dd(c, j).wait_recv()
        p1(CHUNKS - 1, j).wait_send()
        for c in (CHUNKS - 2, CHUNKS - 1):
            p2(c, j).wait_send()
            p3(c, j).wait_send()
            a1(c, j).wait_send()
        for c in range(CHUNKS):
            a2(c, j).wait_send()
            a3(c, j).wait_send()
            dd(c, j).wait_send()


def hand_over(*refs):
    for src, dst in zip(refs[:4], refs[4:]):
        dst[...] = src[...]


def solution(mesh):
    bf = lambda *s: pltpu.VMEM(s, BF)
    dma = lambda *s: pltpu.SemaphoreType.DMA(s)

    def step(x, dy, gate, up, w_gate, w_up, w_down):
        outs = [(ROWS, D), (D, H), (D, H), (H, D), (ROWS, H), (ROWS, H), (ROWS, H)]
        scratch = [pltpu.VMEM((Q1, D), F32), pltpu.VMEM((Q2, D), F32), pltpu.VMEM((Q3, D), F32),
                   bf(HALF, D), bf(2, HALF, D), bf(Q1, D), bf(2, Q1, D), bf(2, Q2, D), bf(2, Q2, D),
                   bf(2, Q3, D), bf(2, Q3, D), bf(2, Q3, D),
                   dma(3), dma(2, 3), dma(3), dma(2, 3), dma(2, 3), dma(2, 3), dma(2, 3), dma(2, 3), dma(2, 3)]
        scratch += [dma(CHUNKS, 3)] * 8
        res = pl.pallas_call(
            kernel,
            in_specs=[pl.BlockSpec(memory_space=pl.ANY)] * 7,
            out_specs=[pl.BlockSpec(memory_space=pl.ANY)] * 7,
            out_shape=[jax.ShapeDtypeStruct(s, BF) for s in outs],
            scratch_shapes=scratch,
            compiler_params=pltpu.CompilerParams(collective_id=0, has_side_effects=True, vmem_limit_bytes=67043328),
        )(x, dy, gate, up, w_gate, w_up, w_down)
        n = 8
        specs = [pl.BlockSpec((ROWS // n, D), lambda i: (i, 0)), pl.BlockSpec((D // n, H), lambda i: (i, 0)),
                 pl.BlockSpec((D // n, H), lambda i: (i, 0)), pl.BlockSpec((H // n, D), lambda i: (i, 0))]
        return pl.pallas_call(
            hand_over,
            grid=(n,),
            in_specs=specs,
            out_specs=specs,
            out_shape=[jax.ShapeDtypeStruct(s, BF) for s in outs[:4]],
            compiler_params=pltpu.CompilerParams(vmem_limit_bytes=60 << 20),
        )(*res[:4])

    tokens, columns, rows = P("dp", None), P(None, "tp"), P("tp", None)
    return jax.shard_map(
        step,
        mesh=mesh,
        in_specs=(tokens, tokens, P("dp", "tp"), P("dp", "tp"), columns, columns, rows),
        out_specs=(tokens, P("dp", "tp"), P("dp", "tp"), P(("dp", "tp"), None)),
        check_vma=False,
    )
```

```python
import functools

import jax
import jax.numpy as jnp
from jax import lax
from jax.experimental import pallas as pl
from jax.experimental.pallas import tpu as pltpu
from jax.sharding import PartitionSpec as P

BF, F32 = jnp.bfloat16, jnp.float32
NT = (((1,), (1,)), ((), ()))
TN = (((0,), (0,)), ((), ()))
MESH = pl.DeviceIdType.MESH

ROWS, D, H = 2048, 5120, 1024
CHUNKS = 4
HALF = ROWS // CHUNKS // 2
Q1, Q2, Q3 = HALF // 2, HALF // 4, HALF // 8
COLS = ((0, 1792), (1792, 1792), (3584, 1536))
TILE = 512
TILES = D // TILE

PLAN1 = {15: [100], 16: [102, 101], 19: [200], 20: [202], 23: [201], 25: [111, 112, 110], 26: [300], 27: [301, 302], 32: [211], 33: [210, 212], 34:
         [400, 401], 35: [120, 122, 121], 36: [310, 311], 38: [312, 402], 39: [222]}
PLAN2 = {1: [220], 2: [221, 501, 131], 3: [130], 4: [322, 321, 411, 500], 5: [410, 320], 6: [231, 132, 230], 9: [422, 412, 502], 10: [331], 11: [420,
         232], 12: [421], 13: [330, 511], 14: [332], 15: [510, 431], 16: [522], 17: [520, 432, 430], 18: [602], 20: [521, 600], 21: [512, 622], 22:
         [531], 23: [530, 532], 24: [611], 25: [601, 610], 26: [612], 27: [620], 29: [621]}
PLAN3 = [632, 631, 630]


def dot(a, b, dims):
    return lax.dot_general(a, b, dims, preferred_element_type=F32)


def kernel(x, dy, gate, up, w_gate, w_up, w_down, dx, dwg, dwu, dwd, dg_o, du_o, hd_o,
           acc1, acc2, acc3, ds_, dr, s1, r1, s2, r2, s3, r3, fin,
           d_s, d_r, p1_s, p1_r, p2_s, p2_r, p3_s, p3_r, loc_s,
           a1_s, a1_r, a2_s, a2_r, a3_s, a3_r, dd_s, dd_r, de_s, de_r):
    me, dp = lax.axis_index("tp"), lax.axis_index("dp")
    core, bz, by, bx = me % 2, me // 2 % 2, me // 4 % 2, me // 8 % 2
    other = me + 1 - 2 * core
    axes = {"x": (bx, me + 8 - 16 * bx), "y": (by, me + 4 - 8 * by), "z": (bz, me + 2 - 4 * bz)}
    orders = [[axes[a] for a in o] for o in ("yzx", "xyz", "zxy")]

    barrier = pltpu.get_barrier_semaphore()
    for peer in (other, axes["x"][1], axes["y"][1], axes["z"][1]):
        pl.semaphore_signal(barrier, inc=1, device_id=(dp, peer), device_id_type=MESH)

    def remote(src, dst, ss, rs, peer):
        return pltpu.make_async_remote_copy(src_ref=src, dst_ref=dst, send_sem=ss, recv_sem=rs,
                                            device_id=(dp, peer), device_id_type=MESH)

    def cols(j):
        return pl.ds(*COLS[j])

    def al(v, n):
        return pl.multiple_of(v, n)

    def base(c):
        return c * (2 * HALF) + HALF * core

    def d_copy(c, j):
        return remote(ds_.at[:, cols(j)], dr.at[c % 2, :, cols(j)], d_s.at[j], d_r.at[c % 2, j], other)

    def p1(c, j):
        return remote(s1.at[:, cols(j)], r1.at[c % 2, :, cols(j)], p1_s.at[j], p1_r.at[c % 2, j], orders[j][0][1])

    def p2(c, j):
        return remote(s2.at[c % 2, :, cols(j)], r2.at[c % 2, :, cols(j)], p2_s.at[c % 2, j], p2_r.at[c % 2, j], orders[j][1][1])

    def p3(c, j):
        return remote(s3.at[c % 2, :, cols(j)], r3.at[c % 2, :, cols(j)], p3_s.at[c % 2, j], p3_r.at[c % 2, j], orders[j][2][1])

    def rows3(c, j):
        b = orders[j]
        return pl.ds(al(base(c) + Q1 * b[0][0] + Q2 * b[1][0] + Q3 * b[2][0], Q3), Q3)

    def rows2(c, j):
        b = orders[j]
        return pl.ds(al(base(c) + Q1 * b[0][0] + Q2 * b[1][0], Q2), Q2)

    def rows1(c, j):
        return pl.ds(al(base(c) + Q1 * orders[j][0][0], Q1), Q1)

    def loc(c, j):
        return pltpu.make_async_copy(fin.at[c % 2, :, cols(j)], dx.at[rows3(c, j), cols(j)], loc_s.at[c % 2, j])

    def a1(c, j):
        return remote(fin.at[c % 2, :, cols(j)], dx.at[rows3(c, j), cols(j)], a1_s.at[c, j], a1_r.at[c, j], orders[j][2][1])

    def a2(c, j):
        r = dx.at[rows2(c, j), cols(j)]
        return remote(r, r, a2_s.at[c, j], a2_r.at[c, j], orders[j][1][1])

    def a3(c, j):
        r = dx.at[rows1(c, j), cols(j)]
        return remote(r, r, a3_s.at[c, j], a3_r.at[c, j], orders[j][0][1])

    def dd(c, j):
        r = dx.at[rows1(c, j), cols(j)]
        return remote(r, r, dd_s.at[c, j], dd_r.at[c, j], other)

    def de(c, j):
        r = dx.at[pl.ds(al(base(c) + Q1 - Q1 * orders[j][0][0], Q1), Q1), cols(j)]
        return remote(r, r, de_s.at[c, j], de_r.at[c, j], other)

    def stage1(c, j):
        bit = orders[j][1][0]
        keep, send = pl.ds(al(Q2 * bit, Q2), Q2), pl.ds(al(Q2 - Q2 * bit, Q2), Q2)
        p1(c, j).wait_recv()
        if c >= 2:
            p2(c - 2, j).wait_send()
        s2[c % 2, :, cols(j)] = (acc1[send, cols(j)] + r1[c % 2, send, cols(j)].astype(F32)).astype(BF)
        p2(c, j).start()
        acc2[:, cols(j)] = acc1[keep, cols(j)] + r1[c % 2, keep, cols(j)].astype(F32)

    def stage2(c, j):
        bit = orders[j][2][0]
        keep, send = pl.ds(al(Q3 * bit, Q3), Q3), pl.ds(al(Q3 - Q3 * bit, Q3), Q3)
        p2(c, j).wait_recv()
        if c >= 2:
            p3(c - 2, j).wait_send()
        s3[c % 2, :, cols(j)] = (acc2[send, cols(j)] + r2[c % 2, send, cols(j)].astype(F32)).astype(BF)
        p3(c, j).start()
        acc3[:, cols(j)] = acc2[keep, cols(j)] + r2[c % 2, keep, cols(j)].astype(F32)

    def stage3(c, j):
        p3(c, j).wait_recv()
        if c >= 2:
            a1(c - 2, j).wait_send()
        fin[c % 2, :, cols(j)] = (acc3[:, cols(j)] + r3[c % 2, :, cols(j)].astype(F32)).astype(BF)
        a1(c, j).start()
        loc(c, j).start()

    def stage4(c, j):
        a1(c, j).wait_recv()
        loc(c, j).wait()
        a2(c, j).start()

    def stage5(c, j):
        a2(c, j).wait_recv()
        a3(c, j).start()
        dd(c, j).start()

    def stage6(c, j):
        a3(c, j).wait_recv()
        de(c, j).start()

    stages = (None, stage1, stage2, stage3, stage4, stage5, stage6)

    def run(codes):
        for code in codes:
            stages[code // 100](code // 10 % 10, code % 10)

    def serve(plan, per_step, step, sub):
        for at, codes in plan.items():
            if at % per_step == sub:
                pl.when(step == at // per_step)(functools.partial(run, codes))

    def terms_phase(wg, wu, wd, dyb, gb, ub, dgb, dub, hdb, ld_w, ld_wd, ld, wr):
        def start_rows(c, h):
            return c * (2 * HALF) + HALF * (core if h else 1 - core)

        def loads(c, h):
            r = pl.ds(al(start_rows(c, h), HALF), HALF)
            return [pltpu.make_async_copy(src.at[r], dst.at[h], ld.at[h, i])
                    for i, (src, dst) in enumerate(((dy, dyb), (gate, gb), (up, ub)))]

        def writes(c, h):
            r = pl.ds(al(start_rows(c, h), HALF), HALF)
            return [pltpu.make_async_copy(src.at[h], dst.at[r], wr.at[h, i])
                    for i, (src, dst) in enumerate(((dgb, dg_o), (dub, du_o), (hdb, hd_o)))]

        def weights(j):
            return [pltpu.make_async_copy(src.at[cols(j)], dst.at[cols(j)], ld_w.at[i, j])
                    for i, (src, dst) in enumerate(((w_gate, wg), (w_up, wu)))]

        halves = [pltpu.make_async_copy(w_down.at[pl.ds(i * (H // 2), H // 2)], wd.at[pl.ds(i * (H // 2), H // 2)], ld_wd.at[i])
                  for i in range(2)]
        for d in loads(0, 0) + halves:
            d.start()
        pl.semaphore_wait(barrier, 4)
        halves[0].wait()
        for d in weights(0):
            d.start()

        def hidden_rows(c, h):
            for d in loads(c, h):
                d.wait()

            @pl.when(c >= 1)
            def _():
                for d in writes(c - 1, h):
                    d.wait()
            for i in range(2):
                part = pl.ds(i * (H // 2), H // 2)
                if h == 0 and i == 1:
                    @pl.when(c == 0)
                    def _():
                        halves[1].wait()
                        for d in loads(0, 1) + weights(1) + weights(2):
                            d.start()
                g, u = gb[h, :, part].astype(F32), ub[h, :, part].astype(F32)
                sig = jax.nn.sigmoid(g)
                silu = g * sig
                hdb[h, :, part] = (silu * u).astype(BF)
                dh = dot(dyb[h], wd[part, :], NT)
                dub[h, :, part] = (dh * silu).astype(BF)
                dgb[h, :, part] = (dh * u * (sig + silu * (1 - sig))).astype(BF)
                if i == 0:
                    serve(PLAN1, 10, c, 5 * h)
            for d in writes(c, h):
                d.start()

            @pl.when(c + 1 < CHUNKS)
            def _():
                for d in loads(c + 1, h):
                    d.start()

        def term(h, j):
            return dot(dgb[h], wg[cols(j), :], NT) + dot(dub[h], wu[cols(j), :], NT)

        def chunk(c, carry):
            hidden_rows(c, 0)
            serve(PLAN1, 10, c, 1)
            for j in range(3):
                @pl.when(c == 0)
                def _():
                    for d in weights(j):
                        d.wait()

                @pl.when(c >= 1)
                def _():
                    d_copy(c - 1, j).wait_send()
                ds_[:, cols(j)] = term(0, j).astype(BF)
                d_copy(c, j).start()
                serve(PLAN1, 10, c, 2 + j)
            hidden_rows(c, 1)
            serve(PLAN1, 10, c, 6)
            for j in range(3):
                d_copy(c, j).wait_recv()

                @pl.when(c >= 1)
                def _():
                    p1(c - 1, j).wait_send()
                t = term(1, j) + dr[c % 2, :, cols(j)].astype(F32)
                high = orders[j][0][0] == 1
                s1[:, cols(j)] = jnp.where(high, t[:Q1], t[Q1:]).astype(BF)
                p1(c, j).start()
                acc1[:, cols(j)] = jnp.where(high, t[Q1:], t[:Q1])
                serve(PLAN1, 10, c, 7 + j)
            return carry

        lax.fori_loop(0, CHUNKS, chunk, 0)
        for h in range(2):
            for d in writes(CHUNKS - 1, h):
                d.wait()
        for j in range(3):
            d_copy(CHUNKS - 1, j).wait_send()

    bf = lambda *s: pltpu.VMEM(s, BF)
    dma = lambda *s: pltpu.SemaphoreType.DMA(s)
    pl.run_scoped(terms_phase, bf(D, H), bf(D, H), bf(H, D), bf(2, HALF, D), bf(2, HALF, H), bf(2, HALF, H),
                  bf(2, HALF, H), bf(2, HALF, H), bf(2, HALF, H), dma(2, 3), dma(2), dma(2, 3), dma(2, 3))

    def weights_phase(dg, du, hd, xb, yb, og, ou, od, ld_f, ld_x, ld_y, wr):
        def tile(t):
            return pl.ds(al(t * TILE, TILE), TILE)

        def load_x(t):
            return pltpu.make_async_copy(x.at[:, tile(t)], xb.at[t % 2], ld_x.at[t % 2])

        def load_y(t):
            return pltpu.make_async_copy(dy.at[:, tile(t)], yb.at[t % 2], ld_y.at[t % 2])

        full = [pltpu.make_async_copy(src, dst, ld_f.at[i])
                for i, (src, dst) in enumerate(((dg_o, dg), (du_o, du), (hd_o, hd)))]

        def write(t, i):
            s = t % 2
            if i == 2:
                return pltpu.make_async_copy(od.at[s], dwd.at[:, tile(t)], wr.at[s, 2])
            src, dst = ((og, dwg), (ou, dwu))[i]
            return pltpu.make_async_copy(src.at[s], dst.at[tile(t)], wr.at[s, i])

        full[0].start()
        load_x(0).start()
        full[1].start()
        full[2].start()
        load_y(0).start()

        def unit(t, carry):
            s = t % 2

            @pl.when(t + 1 < TILES)
            def _():
                load_x(t + 1).start()
                load_y(t + 1).start()

            @pl.when(t >= 2)
            def _():
                for i in range(3):
                    write(t - 2, i).wait()

            for i, (out, full_v) in enumerate(((og, dg), (ou, du), (od, hd))):
                @pl.when(t == 0)
                def _():
                    full[i].wait()
                if i == 0:
                    load_x(t).wait()
                if i == 2:
                    load_y(t).wait()
                    out[s] = dot(full_v[...], yb[s], TN).astype(BF)
                else:
                    out[s] = dot(xb[s], full_v[...], TN).astype(BF)
                write(t, i).start()
                serve(PLAN2, 3, t, i)
            return carry

        lax.fori_loop(0, TILES, unit, 0)
        for t in (TILES - 2, TILES - 1):
            for i in range(3):
                write(t, i).wait()

    pl.run_scoped(weights_phase, bf(ROWS, H), bf(ROWS, H), bf(ROWS, H), bf(2, ROWS, TILE), bf(2, ROWS, TILE),
                  bf(2, TILE, H), bf(2, TILE, H), bf(2, H, TILE), dma(3), dma(2), dma(2), dma(2, 3))

    run(PLAN3)
    for j in range(3):
        for c in range(CHUNKS):
            dd(c, j).wait_recv()
            de(c, j).wait_recv()
        p1(CHUNKS - 1, j).wait_send()
        for c in (CHUNKS - 2, CHUNKS - 1):
            p2(c, j).wait_send()
            p3(c, j).wait_send()
            a1(c, j).wait_send()
        for c in range(CHUNKS):
            a2(c, j).wait_send()
            a3(c, j).wait_send()
            dd(c, j).wait_send()
            de(c, j).wait_send()


def hand_over(*refs):
    for src, dst in zip(refs[:4], refs[4:]):
        dst[...] = src[...]


def solution(mesh):
    bf = lambda *s: pltpu.VMEM(s, BF)
    dma = lambda *s: pltpu.SemaphoreType.DMA(s)

    def step(x, dy, gate, up, w_gate, w_up, w_down):
        outs = [(ROWS, D), (D, H), (D, H), (H, D), (ROWS, H), (ROWS, H), (ROWS, H)]
        scratch = [pltpu.VMEM((Q1, D), F32), pltpu.VMEM((Q2, D), F32), pltpu.VMEM((Q3, D), F32),
                   bf(HALF, D), bf(2, HALF, D), bf(Q1, D), bf(2, Q1, D), bf(2, Q2, D), bf(2, Q2, D),
                   bf(2, Q3, D), bf(2, Q3, D), bf(2, Q3, D),
                   dma(3), dma(2, 3), dma(3), dma(2, 3), dma(2, 3), dma(2, 3), dma(2, 3), dma(2, 3), dma(2, 3)]
        scratch += [dma(CHUNKS, 3)] * 10
        res = pl.pallas_call(
            kernel,
            in_specs=[pl.BlockSpec(memory_space=pl.ANY)] * 7,
            out_specs=[pl.BlockSpec(memory_space=pl.ANY)] * 7,
            out_shape=[jax.ShapeDtypeStruct(s, BF) for s in outs],
            scratch_shapes=scratch,
            compiler_params=pltpu.CompilerParams(collective_id=0, has_side_effects=True, vmem_limit_bytes=67043328),
        )(x, dy, gate, up, w_gate, w_up, w_down)
        n = 8
        specs = [pl.BlockSpec((ROWS // n, D), lambda i: (i, 0)), pl.BlockSpec((D // n, H), lambda i: (i, 0)),
                 pl.BlockSpec((D // n, H), lambda i: (i, 0)), pl.BlockSpec((H // n, D), lambda i: (i, 0))]
        return pl.pallas_call(
            hand_over,
            grid=(n,),
            in_specs=specs,
            out_specs=specs,
            out_shape=[jax.ShapeDtypeStruct(s, BF) for s in outs[:4]],
            compiler_params=pltpu.CompilerParams(vmem_limit_bytes=60 << 20),
        )(*res[:4])

    tokens, columns, rows = P("dp", None), P(None, "tp"), P("tp", None)
    return jax.shard_map(
        step,
        mesh=mesh,
        in_specs=(tokens, tokens, P("dp", "tp"), P("dp", "tp"), columns, columns, rows),
        out_specs=(tokens, P("dp", "tp"), P("dp", "tp"), P(("dp", "tp"), None)),
        check_vma=False,
    )
```

```python
import functools

import jax
import jax.numpy as jnp
from jax import lax
from jax.experimental import pallas as pl
from jax.experimental.pallas import tpu as pltpu
from jax.sharding import PartitionSpec as P

BF, F32 = jnp.bfloat16, jnp.float32
NT = (((1,), (1,)), ((), ()))
TN = (((0,), (0,)), ((), ()))
MESH = pl.DeviceIdType.MESH

ROWS, D, H = 2048, 5120, 1024
CHUNKS = 4
HALF = ROWS // CHUNKS // 2
Q1, Q2, Q3 = HALF // 2, HALF // 4, HALF // 8
COLS = ((0, 1792), (1792, 1792), (3584, 1536))
LAST = 256
TILE = 512
TILES = D // TILE

PLAN1 = {15: [100], 16: [102, 101], 19: [200], 20: [202], 23: [201], 25: [111, 112, 110], 26: [300], 27: [301, 302], 32: [211], 33: [210, 212], 34:
         [400, 401], 35: [120, 122, 121], 36: [310, 311], 38: [312, 402], 39: [222]}
PLAN2 = {1: [220], 2: [221, 501, 131], 3: [130], 4: [322, 321, 411, 500], 5: [410, 320], 6: [231, 132, 230], 9: [422, 412, 502], 10: [331], 11: [420,
         232], 12: [421], 13: [330, 511], 14: [332], 15: [510, 431], 16: [522], 17: [520, 432, 430], 18: [602], 20: [521, 600], 21: [512, 622], 22:
         [531], 23: [530, 532], 24: [611], 25: [601, 610], 26: [612], 27: [620], 29: [621]}
PLAN3 = [632, 631, 630]


def dot(a, b, dims):
    return lax.dot_general(a, b, dims, preferred_element_type=F32)


def kernel(x, dy, gate, up, w_gate, w_up, w_down, dx, dwg, dwu, dwd, dg_o, du_o, hd_o,
           acc1, acc2, acc3, ds_, dr, s1, r1, s2, r2, s3, r3, fin,
           d_s, d_r, p1_s, p1_r, p2_s, p2_r, p3_s, p3_r, loc_s,
           a1_s, a1_r, a2_s, a2_r, a3_s, a3_r, dd_s, dd_r, de_s, de_r):
    me, dp = lax.axis_index("tp"), lax.axis_index("dp")
    core, bz, by, bx = me % 2, me // 2 % 2, me // 4 % 2, me // 8 % 2
    other = me + 1 - 2 * core
    axes = {"x": (bx, me + 8 - 16 * bx), "y": (by, me + 4 - 8 * by), "z": (bz, me + 2 - 4 * bz)}
    orders = [[axes[a] for a in o] for o in ("yzx", "xyz", "zxy")]

    barrier = pltpu.get_barrier_semaphore()
    for peer in (other, axes["x"][1], axes["y"][1], axes["z"][1]):
        pl.semaphore_signal(barrier, inc=1, device_id=(dp, peer), device_id_type=MESH)

    def remote(src, dst, ss, rs, peer):
        return pltpu.make_async_remote_copy(src_ref=src, dst_ref=dst, send_sem=ss, recv_sem=rs,
                                            device_id=(dp, peer), device_id_type=MESH)

    def cols(j):
        return pl.ds(*COLS[j])

    def al(v, n):
        return pl.multiple_of(v, n)

    def base(c):
        return c * (2 * HALF) + HALF * core

    def d_copy(c, j):
        return remote(ds_.at[:, cols(j)], dr.at[c % 2, :, cols(j)], d_s.at[j], d_r.at[c % 2, j], other)

    def p1(c, j):
        return remote(s1.at[:, cols(j)], r1.at[c % 2, :, cols(j)], p1_s.at[j], p1_r.at[c % 2, j], orders[j][0][1])

    def p2(c, j):
        return remote(s2.at[c % 2, :, cols(j)], r2.at[c % 2, :, cols(j)], p2_s.at[c % 2, j], p2_r.at[c % 2, j], orders[j][1][1])

    def p3(c, j):
        return remote(s3.at[c % 2, :, cols(j)], r3.at[c % 2, :, cols(j)], p3_s.at[c % 2, j], p3_r.at[c % 2, j], orders[j][2][1])

    def rows3(c, j):
        b = orders[j]
        return pl.ds(al(base(c) + Q1 * b[0][0] + Q2 * b[1][0] + Q3 * b[2][0], Q3), Q3)

    def rows2(c, j):
        b = orders[j]
        return pl.ds(al(base(c) + Q1 * b[0][0] + Q2 * b[1][0], Q2), Q2)

    def rows1(c, j):
        return pl.ds(al(base(c) + Q1 * orders[j][0][0], Q1), Q1)

    def loc(c, j):
        return pltpu.make_async_copy(fin.at[c % 2, :, cols(j)], dx.at[rows3(c, j), cols(j)], loc_s.at[c % 2, j])

    def a1(c, j):
        return remote(fin.at[c % 2, :, cols(j)], dx.at[rows3(c, j), cols(j)], a1_s.at[c, j], a1_r.at[c, j], orders[j][2][1])

    def a2(c, j):
        r = dx.at[rows2(c, j), cols(j)]
        return remote(r, r, a2_s.at[c, j], a2_r.at[c, j], orders[j][1][1])

    def a3(c, j):
        r = dx.at[rows1(c, j), cols(j)]
        return remote(r, r, a3_s.at[c, j], a3_r.at[c, j], orders[j][0][1])

    def dd(c, j):
        r = dx.at[rows1(c, j), cols(j)]
        return remote(r, r, dd_s.at[c, j], dd_r.at[c, j], other)

    def de(c, j):
        r = dx.at[pl.ds(al(base(c) + Q1 - Q1 * orders[j][0][0], Q1), Q1), cols(j)]
        return remote(r, r, de_s.at[c, j], de_r.at[c, j], other)

    def stage1(c, j):
        bit = orders[j][1][0]
        keep, send = pl.ds(al(Q2 * bit, Q2), Q2), pl.ds(al(Q2 - Q2 * bit, Q2), Q2)
        p1(c, j).wait_recv()
        if c >= 2:
            p2(c - 2, j).wait_send()
        s2[c % 2, :, cols(j)] = (acc1[send, cols(j)] + r1[c % 2, send, cols(j)].astype(F32)).astype(BF)
        p2(c, j).start()
        acc2[:, cols(j)] = acc1[keep, cols(j)] + r1[c % 2, keep, cols(j)].astype(F32)

    def stage2(c, j):
        bit = orders[j][2][0]
        keep, send = pl.ds(al(Q3 * bit, Q3), Q3), pl.ds(al(Q3 - Q3 * bit, Q3), Q3)
        p2(c, j).wait_recv()
        if c >= 2:
            p3(c - 2, j).wait_send()
        s3[c % 2, :, cols(j)] = (acc2[send, cols(j)] + r2[c % 2, send, cols(j)].astype(F32)).astype(BF)
        p3(c, j).start()
        acc3[:, cols(j)] = acc2[keep, cols(j)] + r2[c % 2, keep, cols(j)].astype(F32)

    def stage3(c, j):
        p3(c, j).wait_recv()
        if c >= 2:
            a1(c - 2, j).wait_send()
        fin[c % 2, :, cols(j)] = (acc3[:, cols(j)] + r3[c % 2, :, cols(j)].astype(F32)).astype(BF)
        a1(c, j).start()
        loc(c, j).start()

    def stage4(c, j):
        a1(c, j).wait_recv()
        loc(c, j).wait()
        a2(c, j).start()

    def stage5(c, j):
        a2(c, j).wait_recv()
        a3(c, j).start()
        dd(c, j).start()

    def stage6(c, j):
        a3(c, j).wait_recv()
        de(c, j).start()

    stages = (None, stage1, stage2, stage3, stage4, stage5, stage6)

    def run(codes):
        for code in codes:
            stages[code // 100](code // 10 % 10, code % 10)

    def serve(plan, per_step, step, sub):
        for at, codes in plan.items():
            if at % per_step == sub:
                pl.when(step == at // per_step)(functools.partial(run, codes))

    def terms_phase(wg, wu, wd, dyb, gb, ub, dgb, dub, hdb, ld_w, ld_wd, ld, wr):
        def start_rows(c, h):
            return c * (2 * HALF) + HALF * (core if h else 1 - core)

        def loads(c, h):
            r = pl.ds(al(start_rows(c, h), HALF), HALF)
            return [pltpu.make_async_copy(src.at[r], dst.at[h], ld.at[h, i])
                    for i, (src, dst) in enumerate(((dy, dyb), (gate, gb), (up, ub)))]

        def writes(c, h):
            r = pl.ds(al(start_rows(c, h), HALF), HALF)
            return [pltpu.make_async_copy(src.at[h], dst.at[r], wr.at[h, i])
                    for i, (src, dst) in enumerate(((dgb, dg_o), (dub, du_o), (hdb, hd_o)))]

        def weights(j):
            return [pltpu.make_async_copy(src.at[cols(j)], dst.at[cols(j)], ld_w.at[i, j])
                    for i, (src, dst) in enumerate(((w_gate, wg), (w_up, wu)))]

        halves = [pltpu.make_async_copy(w_down.at[pl.ds(i * (H // 2), H // 2)], wd.at[pl.ds(i * (H // 2), H // 2)], ld_wd.at[i])
                  for i in range(2)]
        for d in loads(0, 0) + halves:
            d.start()
        pl.semaphore_wait(barrier, 4)
        halves[0].wait()
        for d in weights(0):
            d.start()

        def hidden_rows(c, h):
            for d in loads(c, h):
                d.wait()

            @pl.when(c >= 1)
            def _():
                for d in writes(c - 1, h):
                    d.wait()
            for i in range(2):
                part = pl.ds(i * (H // 2), H // 2)
                if h == 0 and i == 1:
                    @pl.when(c == 0)
                    def _():
                        halves[1].wait()
                        for d in loads(0, 1) + weights(1) + weights(2):
                            d.start()
                g, u = gb[h, :, part].astype(F32), ub[h, :, part].astype(F32)
                sig = jax.nn.sigmoid(g)
                silu = g * sig
                hdb[h, :, part] = (silu * u).astype(BF)
                dh = dot(dyb[h], wd[part, :], NT)
                dub[h, :, part] = (dh * silu).astype(BF)
                dgb[h, :, part] = (dh * u * (sig + silu * (1 - sig))).astype(BF)
                if i == 0:
                    serve(PLAN1, 10, c, 5 * h)
            for d in writes(c, h):
                d.start()

            @pl.when(c + 1 < CHUNKS)
            def _():
                for d in loads(c + 1, h):
                    d.start()

        def term(h, at):
            return dot(dgb[h], wg[at, :], NT) + dot(dub[h], wu[at, :], NT)

        def pieces(j):
            start, width = COLS[j]
            return [pl.ds(start, width - LAST), pl.ds(start + width - LAST, LAST)]

        def chunk(c, carry):
            hidden_rows(c, 0)
            serve(PLAN1, 10, c, 1)
            for j in range(3):
                @pl.when(c == 0)
                def _():
                    for d in weights(j):
                        d.wait()

                @pl.when(c >= 1)
                def _():
                    d_copy(c - 1, j).wait_send()
                for at in pieces(j):
                    ds_[:, at] = term(0, at).astype(BF)
                d_copy(c, j).start()
                serve(PLAN1, 10, c, 2 + j)
            hidden_rows(c, 1)
            serve(PLAN1, 10, c, 6)
            for j in range(3):
                d_copy(c, j).wait_recv()

                @pl.when(c >= 1)
                def _():
                    p1(c - 1, j).wait_send()
                high = orders[j][0][0] == 1
                for at in pieces(j):
                    t = term(1, at) + dr[c % 2, :, at].astype(F32)
                    s1[:, at] = jnp.where(high, t[:Q1], t[Q1:]).astype(BF)
                    acc1[:, at] = jnp.where(high, t[Q1:], t[:Q1])
                p1(c, j).start()
                serve(PLAN1, 10, c, 7 + j)
            return carry

        lax.fori_loop(0, CHUNKS, chunk, 0)
        for h in range(2):
            for d in writes(CHUNKS - 1, h):
                d.wait()
        for j in range(3):
            d_copy(CHUNKS - 1, j).wait_send()

    bf = lambda *s: pltpu.VMEM(s, BF)
    dma = lambda *s: pltpu.SemaphoreType.DMA(s)
    pl.run_scoped(terms_phase, bf(D, H), bf(D, H), bf(H, D), bf(2, HALF, D), bf(2, HALF, H), bf(2, HALF, H),
                  bf(2, HALF, H), bf(2, HALF, H), bf(2, HALF, H), dma(2, 3), dma(2), dma(2, 3), dma(2, 3))

    def weights_phase(dg, du, hd, xb, yb, og, ou, od, ld_f, ld_x, ld_y, wr):
        def tile(t):
            return pl.ds(al(t * TILE, TILE), TILE)

        def load_x(t):
            return pltpu.make_async_copy(x.at[:, tile(t)], xb.at[t % 2], ld_x.at[t % 2])

        def load_y(t):
            return pltpu.make_async_copy(dy.at[:, tile(t)], yb.at[t % 2], ld_y.at[t % 2])

        full = [pltpu.make_async_copy(src, dst, ld_f.at[i])
                for i, (src, dst) in enumerate(((dg_o, dg), (du_o, du), (hd_o, hd)))]

        def write(t, i):
            s = t % 2
            if i == 2:
                return pltpu.make_async_copy(od.at[s], dwd.at[:, tile(t)], wr.at[s, 2])
            src, dst = ((og, dwg), (ou, dwu))[i]
            return pltpu.make_async_copy(src.at[s], dst.at[tile(t)], wr.at[s, i])

        full[0].start()
        load_x(0).start()
        full[1].start()
        full[2].start()
        load_y(0).start()

        def unit(t, carry):
            s = t % 2

            @pl.when(t + 1 < TILES)
            def _():
                load_x(t + 1).start()
                load_y(t + 1).start()

            @pl.when(t >= 2)
            def _():
                for i in range(3):
                    write(t - 2, i).wait()

            for i, (out, full_v) in enumerate(((og, dg), (ou, du), (od, hd))):
                @pl.when(t == 0)
                def _():
                    full[i].wait()
                if i == 0:
                    load_x(t).wait()
                if i == 2:
                    load_y(t).wait()
                    out[s] = dot(full_v[...], yb[s], TN).astype(BF)
                else:
                    out[s] = dot(xb[s], full_v[...], TN).astype(BF)
                write(t, i).start()
                serve(PLAN2, 3, t, i)
            return carry

        lax.fori_loop(0, TILES, unit, 0)
        for t in (TILES - 2, TILES - 1):
            for i in range(3):
                write(t, i).wait()

    pl.run_scoped(weights_phase, bf(ROWS, H), bf(ROWS, H), bf(ROWS, H), bf(2, ROWS, TILE), bf(2, ROWS, TILE),
                  bf(2, TILE, H), bf(2, TILE, H), bf(2, H, TILE), dma(3), dma(2), dma(2), dma(2, 3))

    run(PLAN3)
    for j in range(3):
        for c in range(CHUNKS):
            dd(c, j).wait_recv()
            de(c, j).wait_recv()
        p1(CHUNKS - 1, j).wait_send()
        for c in (CHUNKS - 2, CHUNKS - 1):
            p2(c, j).wait_send()
            p3(c, j).wait_send()
            a1(c, j).wait_send()
        for c in range(CHUNKS):
            a2(c, j).wait_send()
            a3(c, j).wait_send()
            dd(c, j).wait_send()
            de(c, j).wait_send()


def hand_over(*refs):
    for src, dst in zip(refs[:4], refs[4:]):
        dst[...] = src[...]


def solution(mesh):
    bf = lambda *s: pltpu.VMEM(s, BF)
    dma = lambda *s: pltpu.SemaphoreType.DMA(s)

    def step(x, dy, gate, up, w_gate, w_up, w_down):
        outs = [(ROWS, D), (D, H), (D, H), (H, D), (ROWS, H), (ROWS, H), (ROWS, H)]
        scratch = [pltpu.VMEM((Q1, D), F32), pltpu.VMEM((Q2, D), F32), pltpu.VMEM((Q3, D), F32),
                   bf(HALF, D), bf(2, HALF, D), bf(Q1, D), bf(2, Q1, D), bf(2, Q2, D), bf(2, Q2, D),
                   bf(2, Q3, D), bf(2, Q3, D), bf(2, Q3, D),
                   dma(3), dma(2, 3), dma(3), dma(2, 3), dma(2, 3), dma(2, 3), dma(2, 3), dma(2, 3), dma(2, 3)]
        scratch += [dma(CHUNKS, 3)] * 10
        res = pl.pallas_call(
            kernel,
            in_specs=[pl.BlockSpec(memory_space=pl.ANY)] * 7,
            out_specs=[pl.BlockSpec(memory_space=pl.ANY)] * 7,
            out_shape=[jax.ShapeDtypeStruct(s, BF) for s in outs],
            scratch_shapes=scratch,
            compiler_params=pltpu.CompilerParams(collective_id=0, has_side_effects=True, vmem_limit_bytes=67043328),
        )(x, dy, gate, up, w_gate, w_up, w_down)
        n = 8
        specs = [pl.BlockSpec((ROWS // n, D), lambda i: (i, 0)), pl.BlockSpec((D // n, H), lambda i: (i, 0)),
                 pl.BlockSpec((D // n, H), lambda i: (i, 0)), pl.BlockSpec((H // n, D), lambda i: (i, 0))]
        return pl.pallas_call(
            hand_over,
            grid=(n,),
            in_specs=specs,
            out_specs=specs,
            out_shape=[jax.ShapeDtypeStruct(s, BF) for s in outs[:4]],
            compiler_params=pltpu.CompilerParams(vmem_limit_bytes=60 << 20),
        )(*res[:4])

    tokens, columns, rows = P("dp", None), P(None, "tp"), P("tp", None)
    return jax.shard_map(
        step,
        mesh=mesh,
        in_specs=(tokens, tokens, P("dp", "tp"), P("dp", "tp"), columns, columns, rows),
        out_specs=(tokens, P("dp", "tp"), P("dp", "tp"), P(("dp", "tp"), None)),
        check_vma=False,
    )
```

```python
import functools

import jax
import jax.numpy as jnp
from jax import lax
from jax.experimental import pallas as pl
from jax.experimental.pallas import tpu as pltpu
from jax.sharding import PartitionSpec as P

BF, F32 = jnp.bfloat16, jnp.float32
NT = (((1,), (1,)), ((), ()))
TN = (((0,), (0,)), ((), ()))
MESH = pl.DeviceIdType.MESH

ROWS, D, H = 2048, 5120, 1024
CHUNKS = 4
HALF = ROWS // CHUNKS // 2
Q1, Q2, Q3 = HALF // 2, HALF // 4, HALF // 8
COLS = ((0, 1792), (1792, 1792), (3584, 1536))
LAST = 256
TILE = 512
TILES = D // TILE

PLAN1 = {15: [100], 16: [102, 101], 19: [200], 20: [202], 23: [201], 25: [111, 112, 110], 26: [300], 27: [301, 302], 32: [211], 33: [210, 212], 34:
         [400, 401], 35: [120, 122, 121], 36: [310, 311], 38: [312, 402], 39: [222]}
PLAN2 = {1: [220], 2: [221, 501, 131], 3: [130], 4: [322, 321, 411, 500], 5: [410, 320], 6: [231, 132, 230], 9: [422, 412, 502], 10: [331], 11: [420,
         232], 12: [421], 13: [330, 511], 14: [332], 15: [510, 431], 16: [522], 17: [520, 432, 430], 18: [602], 20: [521, 600], 21: [512, 622], 22:
         [531], 23: [530, 532], 24: [611], 25: [601, 610], 26: [612], 27: [620], 29: [621]}
PLAN3 = [632, 631, 630]


def dot(a, b, dims):
    return lax.dot_general(a, b, dims, preferred_element_type=F32)


def kernel(x, dy, gate, up, w_gate, w_up, w_down, dx, dwg, dwu, dwd, dg_o, du_o, hd_o,
           acc1, acc2, acc3, ds_, dr, s1, r1, s2, r2, s3, r3, fin,
           d_s, d_r, p1_s, p1_r, p2_s, p2_r, p3_s, p3_r, loc_s,
           a1_s, a1_r, a2_s, a2_r, a3_s, a3_r, dd_s, dd_r, de_s, de_r):
    me, dp = lax.axis_index("tp"), lax.axis_index("dp")
    core, bz, by, bx = me % 2, me // 2 % 2, me // 4 % 2, me // 8 % 2
    other = me + 1 - 2 * core
    axes = {"x": (bx, me + 8 - 16 * bx), "y": (by, me + 4 - 8 * by), "z": (bz, me + 2 - 4 * bz)}
    orders = [[axes[a] for a in o] for o in ("yzx", "xyz", "zxy")]

    barrier = pltpu.get_barrier_semaphore()
    for peer in (other, axes["x"][1], axes["y"][1], axes["z"][1]):
        pl.semaphore_signal(barrier, inc=1, device_id=(dp, peer), device_id_type=MESH)

    def remote(src, dst, ss, rs, peer):
        return pltpu.make_async_remote_copy(src_ref=src, dst_ref=dst, send_sem=ss, recv_sem=rs,
                                            device_id=(dp, peer), device_id_type=MESH)

    def cols(j):
        return pl.ds(*COLS[j])

    def al(v, n):
        return pl.multiple_of(v, n)

    def base(c):
        return c * (2 * HALF) + HALF * core

    def d_copy(c, j):
        return remote(ds_.at[:, cols(j)], dr.at[c % 2, :, cols(j)], d_s.at[j], d_r.at[c % 2, j], other)

    def p1(c, j):
        return remote(s1.at[:, cols(j)], r1.at[c % 2, :, cols(j)], p1_s.at[j], p1_r.at[c % 2, j], orders[j][0][1])

    def p2(c, j):
        return remote(s2.at[c % 2, :, cols(j)], r2.at[c % 2, :, cols(j)], p2_s.at[c % 2, j], p2_r.at[c % 2, j], orders[j][1][1])

    def p3(c, j):
        return remote(s3.at[c % 2, :, cols(j)], r3.at[c % 2, :, cols(j)], p3_s.at[c % 2, j], p3_r.at[c % 2, j], orders[j][2][1])

    def rows3(c, j):
        b = orders[j]
        return pl.ds(al(base(c) + Q1 * b[0][0] + Q2 * b[1][0] + Q3 * b[2][0], Q3), Q3)

    def rows2(c, j):
        b = orders[j]
        return pl.ds(al(base(c) + Q1 * b[0][0] + Q2 * b[1][0], Q2), Q2)

    def rows1(c, j):
        return pl.ds(al(base(c) + Q1 * orders[j][0][0], Q1), Q1)

    def loc(c, j):
        return pltpu.make_async_copy(fin.at[c % 2, :, cols(j)], dx.at[rows3(c, j), cols(j)], loc_s.at[c % 2, j])

    def a1(c, j):
        return remote(fin.at[c % 2, :, cols(j)], dx.at[rows3(c, j), cols(j)], a1_s.at[c, j], a1_r.at[c, j], orders[j][2][1])

    def a2(c, j):
        r = dx.at[rows2(c, j), cols(j)]
        return remote(r, r, a2_s.at[c, j], a2_r.at[c, j], orders[j][1][1])

    def a3(c, j):
        r = dx.at[rows1(c, j), cols(j)]
        return remote(r, r, a3_s.at[c, j], a3_r.at[c, j], orders[j][0][1])

    def dd(c, j):
        r = dx.at[rows1(c, j), cols(j)]
        return remote(r, r, dd_s.at[c, j], dd_r.at[c, j], other)

    def de(c, j):
        r = dx.at[pl.ds(al(base(c) + Q1 - Q1 * orders[j][0][0], Q1), Q1), cols(j)]
        return remote(r, r, de_s.at[c, j], de_r.at[c, j], other)

    def stage1(c, j):
        bit = orders[j][1][0]
        keep, send = pl.ds(al(Q2 * bit, Q2), Q2), pl.ds(al(Q2 - Q2 * bit, Q2), Q2)
        p1(c, j).wait_recv()
        if c >= 2:
            p2(c - 2, j).wait_send()
        s2[c % 2, :, cols(j)] = (acc1[send, cols(j)] + r1[c % 2, send, cols(j)].astype(F32)).astype(BF)
        p2(c, j).start()
        acc2[:, cols(j)] = acc1[keep, cols(j)] + r1[c % 2, keep, cols(j)].astype(F32)

    def stage2(c, j):
        bit = orders[j][2][0]
        keep, send = pl.ds(al(Q3 * bit, Q3), Q3), pl.ds(al(Q3 - Q3 * bit, Q3), Q3)
        p2(c, j).wait_recv()
        if c >= 2:
            p3(c - 2, j).wait_send()
        s3[c % 2, :, cols(j)] = (acc2[send, cols(j)] + r2[c % 2, send, cols(j)].astype(F32)).astype(BF)
        p3(c, j).start()
        acc3[:, cols(j)] = acc2[keep, cols(j)] + r2[c % 2, keep, cols(j)].astype(F32)

    def stage3(c, j):
        p3(c, j).wait_recv()
        if c >= 2:
            a1(c - 2, j).wait_send()
        fin[c % 2, :, cols(j)] = (acc3[:, cols(j)] + r3[c % 2, :, cols(j)].astype(F32)).astype(BF)
        a1(c, j).start()
        loc(c, j).start()

    def stage4(c, j):
        a1(c, j).wait_recv()
        loc(c, j).wait()
        a2(c, j).start()

    def stage5(c, j):
        a2(c, j).wait_recv()
        a3(c, j).start()
        dd(c, j).start()

    def stage6(c, j):
        a3(c, j).wait_recv()
        de(c, j).start()

    stages = (None, stage1, stage2, stage3, stage4, stage5, stage6)

    def run(codes):
        for code in codes:
            stages[code // 100](code // 10 % 10, code % 10)

    def serve(plan, per_step, step, sub):
        for at, codes in plan.items():
            if at % per_step == sub:
                pl.when(step == at // per_step)(functools.partial(run, codes))

    def terms_phase(wg, wu, wd, dyb, gb, ub, dgb, dub, hdb, ld_w, ld_wd, ld, wr):
        def start_rows(c, h):
            return c * (2 * HALF) + HALF * (core if h else 1 - core)

        def loads(c, h):
            r = pl.ds(al(start_rows(c, h), HALF), HALF)
            return [pltpu.make_async_copy(src.at[r], dst.at[h], ld.at[h, i])
                    for i, (src, dst) in enumerate(((dy, dyb), (gate, gb), (up, ub)))]

        def writes(c, h):
            r = pl.ds(al(start_rows(c, h), HALF), HALF)
            return [pltpu.make_async_copy(src.at[h], dst.at[r], wr.at[h, i])
                    for i, (src, dst) in enumerate(((dgb, dg_o), (dub, du_o), (hdb, hd_o)))]

        def weights(j):
            return [pltpu.make_async_copy(src.at[cols(j)], dst.at[cols(j)], ld_w.at[i, j])
                    for i, (src, dst) in enumerate(((w_gate, wg), (w_up, wu)))]

        halves = [pltpu.make_async_copy(w_down.at[pl.ds(i * (H // 2), H // 2)], wd.at[pl.ds(i * (H // 2), H // 2)], ld_wd.at[i])
                  for i in range(2)]
        for d in loads(0, 0) + halves:
            d.start()
        pl.semaphore_wait(barrier, 4)
        halves[0].wait()
        for d in weights(0):
            d.start()

        def hidden_rows(c, h):
            for d in loads(c, h):
                d.wait()

            @pl.when(c >= 1)
            def _():
                for d in writes(c - 1, h):
                    d.wait()
            for i in range(2):
                part = pl.ds(i * (H // 2), H // 2)
                if h == 0 and i == 1:
                    @pl.when(c == 0)
                    def _():
                        halves[1].wait()
                        for d in loads(0, 1) + weights(1) + weights(2):
                            d.start()
                g, u = gb[h, :, part].astype(F32), ub[h, :, part].astype(F32)
                sig = jax.nn.sigmoid(g)
                silu = g * sig
                hdb[h, :, part] = (silu * u).astype(BF)
                dh = dot(dyb[h], wd[part, :], NT)
                dub[h, :, part] = (dh * silu).astype(BF)
                dgb[h, :, part] = (dh * u * (sig + silu * (1 - sig))).astype(BF)
                if i == 0:
                    serve(PLAN1, 10, c, 5 * h)
            for d in writes(c, h):
                d.start()

            @pl.when(c + 1 < CHUNKS)
            def _():
                for d in loads(c + 1, h):
                    d.start()

        def term(h, at):
            return dot(dgb[h], wg[at, :], NT) + dot(dub[h], wu[at, :], NT)

        def pieces(j):
            start, width = COLS[j]
            return [pl.ds(start, 768), pl.ds(start + 768, width - LAST - 768), pl.ds(start + width - LAST, LAST)]

        def chunk(c, carry):
            hidden_rows(c, 0)
            serve(PLAN1, 10, c, 1)
            for j in range(3):
                @pl.when(c == 0)
                def _():
                    for d in weights(j):
                        d.wait()

                @pl.when(c >= 1)
                def _():
                    d_copy(c - 1, j).wait_send()
                for at in pieces(j):
                    ds_[:, at] = term(0, at).astype(BF)
                d_copy(c, j).start()
                serve(PLAN1, 10, c, 2 + j)
            hidden_rows(c, 1)
            serve(PLAN1, 10, c, 6)
            for j in range(3):
                d_copy(c, j).wait_recv()

                @pl.when(c >= 1)
                def _():
                    p1(c - 1, j).wait_send()
                high = orders[j][0][0] == 1
                for at in pieces(j):
                    t = term(1, at) + dr[c % 2, :, at].astype(F32)
                    s1[:, at] = jnp.where(high, t[:Q1], t[Q1:]).astype(BF)
                    acc1[:, at] = jnp.where(high, t[Q1:], t[:Q1])
                p1(c, j).start()
                serve(PLAN1, 10, c, 7 + j)
            return carry

        lax.fori_loop(0, CHUNKS, chunk, 0)
        for h in range(2):
            for d in writes(CHUNKS - 1, h):
                d.wait()
        for j in range(3):
            d_copy(CHUNKS - 1, j).wait_send()

    bf = lambda *s: pltpu.VMEM(s, BF)
    dma = lambda *s: pltpu.SemaphoreType.DMA(s)
    pl.run_scoped(terms_phase, bf(D, H), bf(D, H), bf(H, D), bf(2, HALF, D), bf(2, HALF, H), bf(2, HALF, H),
                  bf(2, HALF, H), bf(2, HALF, H), bf(2, HALF, H), dma(2, 3), dma(2), dma(2, 3), dma(2, 3))

    def weights_phase(dg, du, hd, xb, yb, og, ou, od, ld_f, ld_x, ld_y, wr):
        def tile(t):
            return pl.ds(al(t * TILE, TILE), TILE)

        def load_x(t):
            return pltpu.make_async_copy(x.at[:, tile(t)], xb.at[t % 2], ld_x.at[t % 2])

        def load_y(t):
            return pltpu.make_async_copy(dy.at[:, tile(t)], yb.at[t % 2], ld_y.at[t % 2])

        full = [pltpu.make_async_copy(src, dst, ld_f.at[i])
                for i, (src, dst) in enumerate(((dg_o, dg), (du_o, du), (hd_o, hd)))]

        def write(t, i):
            s = t % 2
            if i == 2:
                return pltpu.make_async_copy(od.at[s], dwd.at[:, tile(t)], wr.at[s, 2])
            src, dst = ((og, dwg), (ou, dwu))[i]
            return pltpu.make_async_copy(src.at[s], dst.at[tile(t)], wr.at[s, i])

        full[0].start()
        load_x(0).start()
        full[1].start()
        full[2].start()
        load_y(0).start()

        def unit(t, carry):
            s = t % 2

            @pl.when(t + 1 < TILES)
            def _():
                load_x(t + 1).start()
                load_y(t + 1).start()

            @pl.when(t >= 2)
            def _():
                for i in range(3):
                    write(t - 2, i).wait()

            for i, (out, full_v) in enumerate(((og, dg), (ou, du), (od, hd))):
                @pl.when(t == 0)
                def _():
                    full[i].wait()
                if i == 0:
                    load_x(t).wait()
                if i == 2:
                    load_y(t).wait()
                    out[s] = dot(full_v[...], yb[s], TN).astype(BF)
                else:
                    out[s] = dot(xb[s], full_v[...], TN).astype(BF)
                write(t, i).start()
                serve(PLAN2, 3, t, i)
            return carry

        lax.fori_loop(0, TILES, unit, 0)
        for t in (TILES - 2, TILES - 1):
            for i in range(3):
                write(t, i).wait()

    pl.run_scoped(weights_phase, bf(ROWS, H), bf(ROWS, H), bf(ROWS, H), bf(2, ROWS, TILE), bf(2, ROWS, TILE),
                  bf(2, TILE, H), bf(2, TILE, H), bf(2, H, TILE), dma(3), dma(2), dma(2), dma(2, 3))

    run(PLAN3)
    for j in range(3):
        for c in range(CHUNKS):
            dd(c, j).wait_recv()
            de(c, j).wait_recv()
        p1(CHUNKS - 1, j).wait_send()
        for c in (CHUNKS - 2, CHUNKS - 1):
            p2(c, j).wait_send()
            p3(c, j).wait_send()
            a1(c, j).wait_send()
        for c in range(CHUNKS):
            a2(c, j).wait_send()
            a3(c, j).wait_send()
            dd(c, j).wait_send()
            de(c, j).wait_send()


def hand_over(*refs):
    for src, dst in zip(refs[:4], refs[4:]):
        dst[...] = src[...]


def solution(mesh):
    bf = lambda *s: pltpu.VMEM(s, BF)
    dma = lambda *s: pltpu.SemaphoreType.DMA(s)

    def step(x, dy, gate, up, w_gate, w_up, w_down):
        outs = [(ROWS, D), (D, H), (D, H), (H, D), (ROWS, H), (ROWS, H), (ROWS, H)]
        scratch = [pltpu.VMEM((Q1, D), F32), pltpu.VMEM((Q2, D), F32), pltpu.VMEM((Q3, D), F32),
                   bf(HALF, D), bf(2, HALF, D), bf(Q1, D), bf(2, Q1, D), bf(2, Q2, D), bf(2, Q2, D),
                   bf(2, Q3, D), bf(2, Q3, D), bf(2, Q3, D),
                   dma(3), dma(2, 3), dma(3), dma(2, 3), dma(2, 3), dma(2, 3), dma(2, 3), dma(2, 3), dma(2, 3)]
        scratch += [dma(CHUNKS, 3)] * 10
        res = pl.pallas_call(
            kernel,
            in_specs=[pl.BlockSpec(memory_space=pl.ANY)] * 7,
            out_specs=[pl.BlockSpec(memory_space=pl.ANY)] * 7,
            out_shape=[jax.ShapeDtypeStruct(s, BF) for s in outs],
            scratch_shapes=scratch,
            compiler_params=pltpu.CompilerParams(collective_id=0, has_side_effects=True, vmem_limit_bytes=67043328),
        )(x, dy, gate, up, w_gate, w_up, w_down)
        n = 8
        specs = [pl.BlockSpec((ROWS // n, D), lambda i: (i, 0)), pl.BlockSpec((D // n, H), lambda i: (i, 0)),
                 pl.BlockSpec((D // n, H), lambda i: (i, 0)), pl.BlockSpec((H // n, D), lambda i: (i, 0))]
        return pl.pallas_call(
            hand_over,
            grid=(n,),
            in_specs=specs,
            out_specs=specs,
            out_shape=[jax.ShapeDtypeStruct(s, BF) for s in outs[:4]],
            compiler_params=pltpu.CompilerParams(vmem_limit_bytes=60 << 20),
        )(*res[:4])

    tokens, columns, rows = P("dp", None), P(None, "tp"), P("tp", None)
    return jax.shard_map(
        step,
        mesh=mesh,
        in_specs=(tokens, tokens, P("dp", "tp"), P("dp", "tp"), columns, columns, rows),
        out_specs=(tokens, P("dp", "tp"), P("dp", "tp"), P(("dp", "tp"), None)),
        check_vma=False,
    )
```
